256 devices in a mesh: grp: 8 (over z), ex: 32 (over y, x, core).
Axes of the slice: x: 4, y: 4, z: 8, core: 2. Of those that a mesh axis runs over, the one named last changes fastest.
Arguments:
- tokens: bfloat16 [16384, 3584], P(('grp', 'ex')), may hold values from -6 to 6
- expert_ids: int32 [16384, 8], P(('grp', 'ex')), may hold values from 0 to 127, all different within a row; in each aligned block of 64 rows (0 to 63, 64 to 127, ...) at most 5 rows name the same one
- combine: float32 [16384, 8], P(('grp', 'ex')), may hold values from 0.25 to 0.5
- hot_flags: int32 [128], replicated, may hold values from 0 to 1
- gate_up_weight: bfloat16 [8, 32, 2, 3584, 512], P('grp', 'ex'), as said below
- gate_up_scale: float32 [8, 32, 2, 28, 512], P('grp', 'ex')
- down_weight: bfloat16 [8, 32, 512, 3584], P('grp', 'ex'), as said below
- down_scale: float32 [8, 32, 4, 3584], P('grp', 'ex')
Outputs:
- moe_out: bfloat16 [16384, 3584], P(('grp', 'ex'))
The draws below stay inside these ranges and needn't reach their ends.
Inputs may be any that keep to these rules, and one draw needn't show every extreme that they name: `expert_ids`: each row names 8 different experts; the 64 rows of one device name one expert at most 5 times. `gate_up_weight`: for an expert whose hot flag is 0, every entry is an integer from -8 to 7. `down_weight`: for an expert whose hot flag is 0, every entry is an integer from -8 to 7.
All inputs are finite; a program needn't handle non-finite values.
Results may differ from the reference program's by a relative error of at most 0.008.
Values may be sent and summed in bfloat16 or wider, within the bound.
No kernel may reach another device: no remote copies, remote signals or barrier semaphores. Data moves between devices by JAX's collectives and lax.ppermute only.
A program may use at most 128 MiB of HBM per device.

```python
import math
import jax
import jax.numpy as jnp
import numpy as np
from jax import lax

D = 3584
FF = 1024
TOP = 8
GROUP = 128
TOK_DEV = 64
SLABS = 8
LANES = 32
EXPERTS = 128
FFH = 512
CAP = 5
TOKENS = 16384
N_GRP = 8
N_EX = 32


def flag_table(key):
    levels = jax.random.randint(jax.random.fold_in(key, 11), (EXPERTS,), 0, 2)
    return levels.astype(jnp.int32)


def slab_flags(key):
    flags = flag_table(key)
    pair_index = jnp.arange(SLABS, dtype=jnp.int32) // 2
    lane_index = jnp.arange(LANES, dtype=jnp.int32)
    return flags[pair_index[:, None] * LANES + lane_index[None, :]]


def mixed_weights(key, shape, fan_in, extra_dims):
    is_hot = slab_flags(key).reshape((SLABS, LANES) + (1,) * extra_dims) == 1
    real_key = jax.random.fold_in(key, 21)
    dense = jax.random.normal(real_key, shape, jnp.float32) * fan_in ** (-0.5)
    codes = jax.random.randint(jax.random.fold_in(key, 22), shape, -8, 8).astype(jnp.float32)
    return jnp.where(is_hot, dense, codes).astype(jnp.bfloat16)


def spread_scales(key, shape, fan_in):
    low_end, high_end = (math.log(0.5), math.log(2.0))
    logs = jax.random.uniform(jax.random.fold_in(key, 31), shape, jnp.float32, low_end, high_end)
    return (jnp.exp(logs) * (0.22 * fan_in ** (-0.5))).astype(jnp.float32)


def draw_hot_flags(key, part):
    return flag_table(key)


def draw_gate_up_weight(key, part):
    return mixed_weights(key, (SLABS, LANES, 2, D, FFH), D, 3)


def draw_down_weight(key, part):
    return mixed_weights(key, (SLABS, LANES, FFH, D), FF, 2)


def draw_gate_up_scale(key, part):
    return spread_scales(key, (SLABS, LANES, 2, D // GROUP, FFH), D)


def draw_down_scale(key, part):
    return spread_scales(key, (SLABS, LANES, FFH // GROUP, D), FF)


def level_of(rng, dims, cuts, low, top_value):
    factor_of = 1.0
    for position, parts in cuts:
        draws = jax.random.uniform(jax.random.fold_in(jax.random.fold_in(rng, 6), position), (parts,), jnp.float32, low / len(cuts), top_value / len(cuts))
        factor_of = factor_of * jnp.repeat(jnp.exp(draws), dims[position] // parts).reshape((-1,) + (1,) * (len(dims) - 1 - position))
    return factor_of


def routed_block(own_key, own, number, rows, number_of, top, reach, skew):
    ranking = jax.random.permutation(own_key, number_of)
    heavy_load, common = shares(number_of, rows * top, reach, skew, True), shares(number_of, rows * top, reach, skew, False)
    places = jnp.arange(number_of)

    def named(sizes, rotation):
        used = int((sizes > 0).sum())
        fixed = max(1, used // 4)
        passed = fixed + (places - fixed + rotation * (used - fixed)) % max(1, number_of - fixed)
        return jnp.zeros((number_of,), jnp.int32).at[ranking[jnp.where(places < fixed, places, passed)]].set(jnp.asarray(sizes, jnp.int32))

    sizes = jnp.where(number % 4 == 0, named(heavy_load, number // 4), named(common, number - number // 4 - 1))
    mixed = jax.random.permutation(jax.random.fold_in(own, 3), number_of)
    source_of, sink = mixed[0:number_of // 2 * 2:2], mixed[1:number_of // 2 * 2:2]
    margin = jnp.minimum(sizes[source_of] - 1, reach - sizes[sink]) // 2
    margin = jnp.where((source_of == ranking[0]) | (sink == ranking[0]) | (sizes[sink] == 0), 0, jnp.maximum(margin, 0))
    passed = jax.random.randint(jax.random.fold_in(own, 4), (number_of // 2,), 0, 1 << 20) % (margin + 1)
    sizes = sizes.at[source_of].add(-passed).at[sink].add(passed)
    labels = jnp.searchsorted(jnp.cumsum(sizes), jnp.arange(rows * top), side="right").astype(jnp.int32)
    grid = labels.reshape(top, rows).T
    grid = grid[jax.random.permutation(jax.random.fold_in(own, 1), rows)]
    rotation = jax.random.randint(jax.random.fold_in(own, 2), (rows, 1), 0, top)
    return jnp.take_along_axis(grid, (jnp.arange(top)[None, :] + rotation) % top, axis=1)


def shares(number_of, total, bound, slope, full):
    weights = [(1 << 20) // math.isqrt(rank ** slope) + 1 for rank in range(1, number_of + 1)]
    largest = bound if full else min(bound, max(-(-total // number_of), total * weights[0] // sum(weights)))
    least = 1 if total - largest >= number_of - 1 else 0
    holding, rest = [largest] + [least] * (number_of - 1), total - largest - least * (number_of - 1)
    while rest > 0:
        movable = [i for i in range(1, number_of) if holding[i] < largest] or [i for i in range(1, number_of) if holding[i] < bound]
        pool, remaining = sum([weights[i] for i in movable]), rest
        for i in movable:
            more = min(bound - holding[i], max(1, remaining * weights[i] // pool), rest)
            holding[i] = holding[i] + more
            rest = rest - more
    return np.array(holding)


def normal_values(stream_key, dims, scale, reach, shards=(), kind=jnp.bfloat16):
    factor_of = level_of(stream_key, dims, shards, -0.22, 0.18) if shards else 1.0
    array = jax.random.normal(stream_key, dims, jnp.float32) * scale * factor_of
    return jnp.minimum(jnp.maximum(array, -reach), reach).astype(kind)


def setup_inputs(seed: int = 0) -> dict:
    key_list = jax.random.split(jax.random.key(seed), 9)
    tokens = normal_values(key_list[0], (TOKENS, D), 1.0, 6.0, ((0, 256),))
    expert_ids_keys = jax.random.split(jax.random.fold_in(key_list[1], 1), TOKENS // TOK_DEV)
    expert_ids_turns = jax.random.permutation(jax.random.fold_in(key_list[1], 3), TOKENS // TOK_DEV)
    expert_ids = jax.vmap(lambda own, number: routed_block(jax.random.fold_in(key_list[1], 2), own, number, TOK_DEV, EXPERTS, TOP, CAP, 2))(expert_ids_keys, expert_ids_turns).reshape((TOKENS, TOP))
    combine = jnp.clip(0.25 + 0.25 * jax.random.uniform(key_list[2], (TOKENS, TOP), jnp.float32) ** level_of(key_list[2], (TOKENS, TOP), ((0, 256),), -0.2, 0.2), 0.25, 0.5)
    hot_flags = draw_hot_flags(jax.random.fold_in(key_list[8], 71), 0)
    gate_up_weight = draw_gate_up_weight(jax.random.fold_in(key_list[8], 71), 0)
    gate_up_scale = draw_gate_up_scale(jax.random.fold_in(key_list[8], 71), 0)
    down_weight = draw_down_weight(jax.random.fold_in(key_list[8], 71), 0)
    down_scale = draw_down_scale(jax.random.fold_in(key_list[8], 71), 0)
    return {"tokens": tokens, "expert_ids": expert_ids, "combine": combine, "hot_flags": hot_flags, "gate_up_weight": gate_up_weight, "gate_up_scale": gate_up_scale, "down_weight": down_weight, "down_scale": down_scale}


def scale_groups(weights, scales):
    row_count = weights.shape[0]
    group_count = scales.shape[0]
    shaped = weights.reshape(group_count, row_count // group_count, weights.shape[1])
    return (shaped * scales[:, None, :]).reshape(weights.shape)


def dequantize(weights, scales, is_hot):
    scaled = scale_groups(weights, scales).astype(jnp.bfloat16)
    return jnp.where(is_hot, weights, scaled)


def half_expert(token_rows, gate_up, gate_up_scales, down, down_scales, is_hot):
    gate_matrix = dequantize(gate_up[0], gate_up_scales[0], is_hot)
    up_matrix = dequantize(gate_up[1], gate_up_scales[1], is_hot)
    down_matrix = dequantize(down, down_scales, is_hot)
    gate_proj = jnp.dot(token_rows, gate_matrix, preferred_element_type=jnp.float32)
    up_proj = jnp.dot(token_rows, up_matrix, preferred_element_type=jnp.float32)
    hidden = (jax.nn.silu(gate_proj) * up_proj).astype(jnp.bfloat16)
    return jnp.dot(hidden, down_matrix, preferred_element_type=jnp.float32).astype(jnp.bfloat16)


def reference(tokens, expert_ids, combine, hot_flags, gate_up_weight, gate_up_scale, down_weight, down_scale):
    lane_count = N_EX
    expert_count = N_GRP * N_EX // 2
    most_rows = N_GRP * N_EX * CAP
    route_total = TOKENS * TOP
    flat_expert = expert_ids.reshape(route_total)
    flat_token = (jnp.arange(route_total, dtype=jnp.int32) // TOP).astype(jnp.int32)
    flat_weight = combine.reshape(route_total)
    padded_tokens = jnp.concatenate([tokens, jnp.zeros((1, D), tokens.dtype)], axis=0)

    def one_expert(running, expert_id):
        picked = jnp.nonzero(flat_expert == expert_id, size=most_rows, fill_value=route_total)[0].astype(jnp.int32)
        is_valid = picked < route_total
        safe_index = jnp.minimum(picked, route_total - 1).astype(jnp.int32)
        token_index = jnp.where(is_valid, flat_token[safe_index], TOKENS).astype(jnp.int32)
        weights_now = jnp.where(is_valid, flat_weight[safe_index], jnp.zeros((), flat_weight.dtype))
        token_rows = padded_tokens[token_index]
        pair_index = expert_id // lane_count
        lane_index = expert_id % lane_count
        is_hot = hot_flags[expert_id] == 1
        half_sum = jnp.zeros((most_rows, D), jnp.float32)
        for half_index in range(2):
            slab_index = 2 * pair_index + half_index
            partial_value = half_expert(token_rows, gate_up_weight[slab_index, lane_index], gate_up_scale[slab_index, lane_index], down_weight[slab_index, lane_index], down_scale[slab_index, lane_index], is_hot)
            half_sum = half_sum + partial_value.astype(jnp.float32)
        rounded = lax.optimization_barrier(half_sum.astype(jnp.bfloat16)).astype(jnp.float32)
        return running.at[token_index].add(weights_now[:, None] * rounded, mode="drop"), None

    running, unused = lax.scan(one_expert, jnp.zeros((TOKENS, D), jnp.float32), jnp.arange(expert_count, dtype=jnp.int32))
    return running.astype(jnp.bfloat16)
```

```python
import jax
import jax.numpy as jnp
from jax import lax
from jax.sharding import PartitionSpec as P

CHUNKS = 4
CAP = 5


def dequantize(weights, scales, is_hot):
    group_count = scales.shape[0]
    shaped = weights.reshape(group_count, weights.shape[0] // group_count, weights.shape[1])
    scaled = (shaped * scales[:, None, :]).reshape(weights.shape).astype(jnp.bfloat16)
    return jnp.where(is_hot, weights, scaled)


def shards(
    tokens, expert_ids, combine, hot_flags, gate_up_weight, gate_up_scale, down_weight, down_scale
):
    group_count = lax.axis_size("grp")
    lane_count = lax.axis_size("ex")
    token_count, model_width = tokens.shape
    top_count = expert_ids.shape[1]
    route_count = token_count * top_count
    block = group_count * CAP
    slot_count = lane_count * block
    column_tokens = group_count * token_count
    own_grp = lax.axis_index("grp")
    own_pair = own_grp // 2
    width = model_width // CHUNKS

    flat_expert = expert_ids.reshape(route_count)
    route_order = jnp.arange(route_count, dtype=jnp.int32)
    earlier = (flat_expert[None, :] == flat_expert[:, None]) & (
        route_order[None, :] < route_order[:, None]
    )
    route_rank = jnp.sum(earlier, axis=1, dtype=jnp.int32)
    code = flat_expert * block + own_grp * CAP + route_rank
    meta = jnp.concatenate(
        [code.reshape(token_count, top_count).astype(jnp.float32), combine], axis=1
    )
    meta = lax.all_gather(meta, "grp", axis=0, tiled=True)
    slot = meta[:, :top_count].astype(jnp.int32) - own_pair * slot_count
    weight = meta[:, top_count:]

    column = [
        lax.all_gather(tokens[:, c * width : (c + 1) * width], "grp", axis=0, tiled=True)
        for c in range(CHUNKS)
    ]

    slots_down = lax.broadcasted_iota(jnp.int32, (slot_count, column_tokens), 0)
    slots_across = lax.broadcasted_iota(jnp.int32, (column_tokens, slot_count), 1)
    slot_t = slot.T
    pick = jnp.zeros((slot_count, column_tokens), jnp.bool_)
    mix = jnp.zeros((column_tokens, slot_count), jnp.float32)
    for k in range(top_count):
        pick = pick | (slot_t[k][None, :] == slots_down)
        mix = jnp.where(slot[:, k][:, None] == slots_across, weight[:, k][:, None], mix)
    pick = pick.astype(jnp.bfloat16)
    mix = mix.astype(jnp.bfloat16)

    is_hot = hot_flags[own_pair * lane_count + lax.axis_index("ex")] == 1
    gate_matrix = dequantize(gate_up_weight[0, 0, 0], gate_up_scale[0, 0, 0], is_hot)
    up_matrix = dequantize(gate_up_weight[0, 0, 1], gate_up_scale[0, 0, 1], is_hot)
    down_matrix = dequantize(down_weight[0, 0], down_scale[0, 0], is_hot)

    def exchange(rows):
        return lax.all_to_all(
            rows.reshape(lane_count, block, width), "ex", split_axis=0, concat_axis=0, tiled=True
        ).reshape(slot_count, width)

    gate = up = 0.0
    for c in range(CHUNKS):
        rows = jnp.dot(pick, column[c], preferred_element_type=jnp.float32).astype(jnp.bfloat16)
        rows = exchange(rows)
        part = slice(c * width, (c + 1) * width)
        gate = gate + jnp.dot(rows, gate_matrix[part], preferred_element_type=jnp.float32)
        up = up + jnp.dot(rows, up_matrix[part], preferred_element_type=jnp.float32)
    hidden = (jax.nn.silu(gate) * up).astype(jnp.bfloat16)

    outs = []
    for c in range(CHUNKS):
        part = slice(c * width, (c + 1) * width)
        rows = jnp.dot(hidden, down_matrix[:, part], preferred_element_type=jnp.float32)
        rows = exchange(rows.astype(jnp.bfloat16))
        sums = jnp.dot(mix, rows, preferred_element_type=jnp.float32).astype(jnp.bfloat16)
        outs.append(lax.psum_scatter(sums, "grp", scatter_dimension=0, tiled=True))
    return jnp.concatenate(outs, axis=1)


def solution(mesh):
    return jax.shard_map(
        shards,
        mesh=mesh,
        in_specs=(
            P(("grp", "ex"), None),
            P(("grp", "ex"), None),
            P(("grp", "ex"), None),
            P(),
            P("grp", "ex", None, None, None),
            P("grp", "ex", None, None, None),
            P("grp", "ex", None, None),
            P("grp", "ex", None, None),
        ),
        out_specs=P(("grp", "ex"), None),
        check_vma=False,
    )
```

```python
import jax
import jax.numpy as jnp
from jax import lax
from jax.sharding import PartitionSpec as P


CAP = 5
HALF = 768
BOTH = 2 * HALF


def dequantize(weights, scales, is_hot):
    group_count = scales.shape[0]
    shaped = weights.reshape(group_count, weights.shape[0] // group_count, weights.shape[1])
    scaled = (shaped * scales[:, None, :]).reshape(weights.shape).astype(jnp.bfloat16)
    return jnp.where(is_hot, weights, scaled)


def matmul(a, b):
    return jnp.dot(a, b, preferred_element_type=jnp.float32)


def shards(
    tokens, expert_ids, combine, hot_flags, gate_up_weight, gate_up_scale, down_weight, down_scale
):
    group_count = lax.axis_size("grp")
    lane_count = lax.axis_size("ex")
    token_count, _ = tokens.shape
    top_count = expert_ids.shape[1]
    route_count = token_count * top_count
    block = group_count * CAP
    slot_count = lane_count * block
    column_tokens = group_count * token_count
    own_grp = lax.axis_index("grp")
    own_pair = own_grp // 2
    own_start = own_grp % 2 * HALF
    other_start = HALF - own_start
    partners = [(g, g ^ 1) for g in range(group_count)]

    flat_expert = expert_ids.reshape(route_count)
    route_order = jnp.arange(route_count, dtype=jnp.int32)
    earlier = (flat_expert[None, :] == flat_expert[:, None]) & (
        route_order[None, :] < route_order[:, None]
    )
    route_rank = jnp.sum(earlier, axis=1, dtype=jnp.int32)

    routes = jnp.concatenate(
        [
            expert_ids.astype(jnp.bfloat16),
            route_rank.reshape(token_count, top_count).astype(jnp.bfloat16),
            combine.astype(jnp.bfloat16),
        ],
        axis=1,
    )
    routes = jnp.pad(routes, ((0, 0), (0, 128 - 3 * top_count)))
    first = jnp.stack(
        [
            jnp.concatenate([tokens[:, start : start + HALF], routes], axis=1)
            for start in (0, HALF)
        ]
    )
    first = jnp.broadcast_to(first[None], (group_count // 2,) + first.shape)
    first = first.reshape(group_count, token_count, HALF + 128)
    first = lax.all_to_all(first, "grp", split_axis=0, concat_axis=0, tiled=True)
    first = first.reshape(column_tokens, HALF + 128)
    rest = lax.all_gather(tokens[:, BOTH:], "grp", axis=0, tiled=True)

    routes = first[:, HALF:]
    expert = routes[:, :top_count].astype(jnp.int32)
    rank = routes[:, top_count : 2 * top_count].astype(jnp.int32)
    weight = routes[:, 2 * top_count : 3 * top_count].astype(jnp.float32)
    source = jnp.arange(column_tokens, dtype=jnp.int32)[:, None] // token_count
    slot = (expert - own_pair * lane_count) * block + source * CAP + rank

    slots_down = lax.broadcasted_iota(jnp.int32, (slot_count, column_tokens), 0)
    slots_across = lax.broadcasted_iota(jnp.int32, (column_tokens, slot_count), 1)
    slot_t = slot.T
    pick = jnp.zeros((slot_count, column_tokens), jnp.bool_)
    mix = jnp.zeros((column_tokens, slot_count), jnp.float32)
    for k in range(top_count):
        pick = pick | (slot_t[k][None, :] == slots_down)
        mix = jnp.where(slot[:, k][:, None] == slots_across, weight[:, k][:, None], mix)
    pick = pick.astype(jnp.bfloat16)
    mix = mix.astype(jnp.bfloat16)

    is_hot = hot_flags[own_pair * lane_count + lax.axis_index("ex")] == 1
    gate_matrix = dequantize(gate_up_weight[0, 0, 0], gate_up_scale[0, 0, 0], is_hot)
    up_matrix = dequantize(gate_up_weight[0, 0, 1], gate_up_scale[0, 0, 1], is_hot)
    down_matrix = dequantize(down_weight[0, 0], down_scale[0, 0], is_hot)

    def exchange(rows):
        return lax.all_to_all(
            rows.reshape(lane_count, block, -1), "ex", split_axis=0, concat_axis=0, tiled=True
        ).reshape(slot_count, -1)

    own_rows = matmul(pick, first[:, :HALF]).astype(jnp.bfloat16)
    own_rows = exchange(own_rows)
    other_rows = lax.ppermute(own_rows, "grp", partners)
    rest_rows = matmul(pick, rest).astype(jnp.bfloat16)
    rest_rows = exchange(rest_rows)

    def project(matrix):
        return (
            matmul(own_rows, lax.dynamic_slice_in_dim(matrix, own_start, HALF, 0))
            + matmul(other_rows, lax.dynamic_slice_in_dim(matrix, other_start, HALF, 0))
            + matmul(rest_rows, matrix[BOTH:])
        )

    gate = project(gate_matrix)
    up = project(up_matrix)
    hidden = (jax.nn.silu(gate) * up).astype(jnp.bfloat16)

    rest_rows = matmul(hidden, down_matrix[:, BOTH:]).astype(jnp.bfloat16)
    rest_rows = exchange(rest_rows)
    other_rows = matmul(
        hidden, lax.dynamic_slice_in_dim(down_matrix, other_start, HALF, 1)
    ).astype(jnp.bfloat16)
    partner_rows = lax.ppermute(other_rows, "grp", partners)
    own_rows = matmul(
        hidden, lax.dynamic_slice_in_dim(down_matrix, own_start, HALF, 1)
    ).astype(jnp.bfloat16)
    own_rows = own_rows.astype(jnp.float32) + partner_rows.astype(jnp.float32)
    own_rows = own_rows.astype(jnp.bfloat16)
    own_rows = exchange(own_rows)
    rest_sums = matmul(mix, rest_rows).astype(jnp.bfloat16)
    rest_out = lax.psum_scatter(rest_sums, "grp", scatter_dimension=0, tiled=True)
    own_sums = matmul(mix, own_rows).astype(jnp.bfloat16)
    own_sums = own_sums.reshape(group_count, token_count, HALF)
    sums = lax.all_to_all(own_sums, "grp", split_axis=0, concat_axis=0, tiled=True)
    sums = sums.reshape(group_count // 2, 2, token_count, HALF).astype(jnp.float32)
    sums = jnp.sum(sums, axis=0).astype(jnp.bfloat16)
    return jnp.concatenate([sums[0], sums[1], rest_out], axis=1)


def solution(mesh):
    return jax.shard_map(
        shards,
        mesh=mesh,
        in_specs=(
            P(("grp", "ex"), None),
            P(("grp", "ex"), None),
            P(("grp", "ex"), None),
            P(),
            P("grp", "ex", None, None, None),
            P("grp", "ex", None, None, None),
            P("grp", "ex", None, None),
            P("grp", "ex", None, None),
        ),
        out_specs=P(("grp", "ex"), None),
        check_vma=False,
    )
```

```python
import jax
import jax.numpy as jnp
from jax import lax
from jax.experimental import pallas as pl
from jax.experimental.pallas import tpu as pltpu
from jax.sharding import PartitionSpec as P


CAP = 5
HALF = 768
BOTH = 2 * HALF
HALF_BACK = 896
BOTH_BACK = 2 * HALF_BACK


def dequantize(weights, scales, is_hot):
    group_count = scales.shape[0]
    shaped = weights.reshape(group_count, weights.shape[0] // group_count, weights.shape[1])
    scaled = (shaped * scales[:, None, :]).reshape(weights.shape).astype(jnp.bfloat16)
    return jnp.where(is_hot, weights, scaled)


def matmul(a, b):
    return jnp.dot(a, b, preferred_element_type=jnp.float32)


def expert_kernel(
    rows, gate_early, up_early, gate_matrix, up_matrix, down_rest, down_other, hidden, rest, other
):
    gate = gate_early[...] + matmul(rows[...], gate_matrix[...])
    up = up_early[...] + matmul(rows[...], up_matrix[...])
    hidden[...] = (gate / (1.0 + jnp.exp(-gate)) * up).astype(jnp.bfloat16)
    other[...] = matmul(hidden[...], down_other[...]).astype(jnp.bfloat16)
    rest[...] = matmul(hidden[...], down_rest[...]).astype(jnp.bfloat16)


def expert_rest(rows, gate_early, up_early, gate_matrix, up_matrix, down_rest, down_other):
    count, depth = rows.shape
    units = gate_matrix.shape[1]
    widths = [units, down_rest.shape[1], down_other.shape[1]]
    width = sum(widths[1:])
    tile = 256

    def tiled(columns):
        return pl.BlockSpec((tile, columns), lambda i: (i, 0))

    def whole(array):
        return pl.BlockSpec(array.shape, lambda i: (0, 0))

    return pl.pallas_call(
        expert_kernel,
        grid=(count // tile,),
        in_specs=[
            tiled(depth),
            tiled(units),
            tiled(units),
            whole(gate_matrix),
            whole(up_matrix),
            whole(down_rest),
            whole(down_other),
        ],
        out_specs=[tiled(columns) for columns in widths],
        out_shape=[jax.ShapeDtypeStruct((count, columns), jnp.bfloat16) for columns in widths],
        compiler_params=pltpu.CompilerParams(
            dimension_semantics=("arbitrary",)
        ),
        cost_estimate=pl.CostEstimate(
            flops=2 * count * units * (2 * depth + width),
            bytes_accessed=2 * (count * (depth + width + 5 * units) + units * (2 * depth + width)),
            transcendentals=count * units,
        ),
        name="expert_rest",
    )(rows, gate_early, up_early, gate_matrix, up_matrix, down_rest, down_other)


def shards(
    tokens, expert_ids, combine, hot_flags, gate_up_weight, gate_up_scale, down_weight, down_scale
):
    group_count = lax.axis_size("grp")
    lane_count = lax.axis_size("ex")
    token_count, model_width = tokens.shape
    top_count = expert_ids.shape[1]
    route_count = token_count * top_count
    block = group_count * CAP
    slot_count = lane_count * block
    column_tokens = group_count * token_count
    own_grp = lax.axis_index("grp")
    own_pair = own_grp // 2
    parity = own_grp % 2
    partners = [(g, g ^ 1) for g in range(group_count)]

    flat_expert = expert_ids.reshape(route_count)
    route_order = jnp.arange(route_count, dtype=jnp.int32)
    earlier = (flat_expert[None, :] == flat_expert[:, None]) & (
        route_order[None, :] < route_order[:, None]
    )
    route_rank = jnp.sum(earlier, axis=1, dtype=jnp.int32)

    routes = jnp.concatenate(
        [
            expert_ids.astype(jnp.bfloat16),
            route_rank.reshape(token_count, top_count).astype(jnp.bfloat16),
            combine.astype(jnp.bfloat16),
        ],
        axis=1,
    )
    routes = jnp.pad(routes, ((0, 0), (0, 128 - 3 * top_count)))
    first = jnp.stack(
        [
            jnp.concatenate([tokens[:, start : start + HALF], routes], axis=1)
            for start in (0, HALF)
        ]
    )
    first = jnp.broadcast_to(first[None], (group_count // 2,) + first.shape)
    first = first.reshape(group_count, token_count, HALF + 128)
    first = lax.all_to_all(first, "grp", split_axis=0, concat_axis=0, tiled=True)
    first = first.reshape(column_tokens, HALF + 128)
    rest = lax.all_gather(tokens[:, BOTH:], "grp", axis=0, tiled=True)

    routes = first[:, HALF:]
    expert = routes[:, :top_count].astype(jnp.int32)
    rank = routes[:, top_count : 2 * top_count].astype(jnp.int32)
    weight = routes[:, 2 * top_count : 3 * top_count].astype(jnp.float32)
    source = jnp.arange(column_tokens, dtype=jnp.int32)[:, None] // token_count
    slot = (expert - own_pair * lane_count) * block + source * CAP + rank

    slots_down = lax.broadcasted_iota(jnp.int32, (slot_count, column_tokens), 0)
    slots_across = lax.broadcasted_iota(jnp.int32, (column_tokens, slot_count), 1)
    slot_t = slot.T
    pick = jnp.zeros((slot_count, column_tokens), jnp.bool_)
    for k in range(top_count):
        pick = pick | (slot_t[k][None, :] == slots_down)
    pick = pick.astype(jnp.bfloat16)
    mix = jnp.zeros((column_tokens, slot_count), jnp.float32)
    for k in range(top_count):
        mix = jnp.where(slot[:, k][:, None] == slots_across, weight[:, k][:, None], mix)
    mix = lax.optimization_barrier(mix.astype(jnp.bfloat16))

    is_hot = hot_flags[own_pair * lane_count + lax.axis_index("ex")] == 1
    group = model_width // gate_up_scale.shape[3]

    def dequantize_gate_up(j, start, stop):
        return dequantize(
            gate_up_weight[0, 0, j, start:stop],
            gate_up_scale[0, 0, j, start // group : stop // group],
            is_hot,
        )

    first_matrices = [dequantize_gate_up(j, 0, BOTH) for j in range(2)]
    rest_matrices = [dequantize_gate_up(j, BOTH, model_width) for j in range(2)]
    down_first = dequantize(
        down_weight[0, 0, :, :BOTH_BACK], down_scale[0, 0, :, :BOTH_BACK], is_hot
    )
    down_rest = dequantize(
        down_weight[0, 0, :, BOTH_BACK:], down_scale[0, 0, :, BOTH_BACK:], is_hot
    )

    def exchange(rows):
        return lax.all_to_all(
            rows.reshape(lane_count, block, -1), "ex", split_axis=0, concat_axis=0, tiled=True
        ).reshape(slot_count, -1)

    own_rows = matmul(pick, first[:, :HALF]).astype(jnp.bfloat16)
    own_rows = exchange(own_rows)
    other_rows = lax.ppermute(own_rows, "grp", partners)
    rest_rows = matmul(pick, rest).astype(jnp.bfloat16)
    rest_rows = exchange(rest_rows)

    early = [
        matmul(own_rows, lax.dynamic_slice_in_dim(matrix, parity * HALF, HALF, 0))
        + matmul(other_rows, lax.dynamic_slice_in_dim(matrix, (1 - parity) * HALF, HALF, 0))
        for matrix in first_matrices
    ]
    early = lax.optimization_barrier(early)
    hidden, rest_rows, other_rows = expert_rest(
        rest_rows,
        *early,
        *rest_matrices,
        down_rest,
        lax.dynamic_slice_in_dim(down_first, (1 - parity) * HALF_BACK, HALF_BACK, 1),
    )
    rest_rows = exchange(rest_rows)
    partner_rows = lax.ppermute(other_rows, "grp", partners)
    own_rows = matmul(
        hidden, lax.dynamic_slice_in_dim(down_first, parity * HALF_BACK, HALF_BACK, 1)
    ).astype(jnp.bfloat16)
    own_rows = lax.optimization_barrier(own_rows)
    own_rows = own_rows.astype(jnp.float32) + partner_rows.astype(jnp.float32)
    own_rows = own_rows.astype(jnp.bfloat16)
    own_rows = exchange(own_rows)
    rest_sums = matmul(mix, rest_rows).astype(jnp.bfloat16)
    rest_out = lax.psum_scatter(rest_sums, "grp", scatter_dimension=0, tiled=True)
    own_sums = matmul(mix, own_rows).astype(jnp.bfloat16)
    own_sums = own_sums.reshape(group_count, token_count, HALF_BACK)
    sums = lax.all_to_all(own_sums, "grp", split_axis=0, concat_axis=0, tiled=True)
    sums = sums.reshape(group_count // 2, 2, token_count, HALF_BACK).astype(jnp.float32)
    sums = jnp.sum(sums, axis=0).astype(jnp.bfloat16)
    return jnp.concatenate([sums[0], sums[1], rest_out], axis=1)


def solution(mesh):
    return jax.shard_map(
        shards,
        mesh=mesh,
        in_specs=(
            P(("grp", "ex"), None),
            P(("grp", "ex"), None),
            P(("grp", "ex"), None),
            P(),
            P("grp", "ex", None, None, None),
            P("grp", "ex", None, None, None),
            P("grp", "ex", None, None),
            P("grp", "ex", None, None),
        ),
        out_specs=P(("grp", "ex"), None),
        check_vma=False,
    )
```

```python
import functools

import jax
import jax.numpy as jnp
from jax import lax
from jax.experimental import pallas as pl
from jax.experimental.pallas import tpu as pltpu
from jax.sharding import PartitionSpec as P


CAP = 5
HALF = 768
BOTH = 2 * HALF
HALF_BACK = 896
BOTH_BACK = 2 * HALF_BACK


def dequantize(weights, scales, is_hot):
    group_count = scales.shape[0]
    shaped = weights.reshape(group_count, weights.shape[0] // group_count, weights.shape[1])
    scaled = (shaped * scales[:, None, :]).reshape(weights.shape).astype(jnp.bfloat16)
    return jnp.where(is_hot, weights, scaled)


def matmul(a, b):
    return jnp.dot(a, b, preferred_element_type=jnp.float32)


def expert_kernel(
    rows, gate_early, up_early, gate_matrix, up_matrix, down_rest, down_other, hidden, rest, other
):
    gate = gate_early[...] + matmul(rows[...], gate_matrix[...])
    up = up_early[...] + matmul(rows[...], up_matrix[...])
    hidden[...] = (gate / (1.0 + jnp.exp(-gate)) * up).astype(jnp.bfloat16)
    other[...] = matmul(hidden[...], down_other[...]).astype(jnp.bfloat16)
    rest[...] = matmul(hidden[...], down_rest[...]).astype(jnp.bfloat16)


def expert_rest(rows, gate_early, up_early, gate_matrix, up_matrix, down_rest, down_other):
    count, depth = rows.shape
    units = gate_matrix.shape[1]
    widths = [units, down_rest.shape[1], down_other.shape[1]]
    width = sum(widths[1:])
    tile = 256

    def tiled(columns):
        return pl.BlockSpec((tile, columns), lambda i: (i, 0))

    def whole(array):
        return pl.BlockSpec(array.shape, lambda i: (0, 0))

    return pl.pallas_call(
        expert_kernel,
        grid=(count // tile,),
        in_specs=[
            tiled(depth),
            tiled(units),
            tiled(units),
            whole(gate_matrix),
            whole(up_matrix),
            whole(down_rest),
            whole(down_other),
        ],
        out_specs=[tiled(columns) for columns in widths],
        out_shape=[jax.ShapeDtypeStruct((count, columns), jnp.bfloat16) for columns in widths],
        compiler_params=pltpu.CompilerParams(
            dimension_semantics=("arbitrary",)
        ),
        cost_estimate=pl.CostEstimate(
            flops=2 * count * units * (2 * depth + width),
            bytes_accessed=2 * (count * (depth + width + 5 * units) + units * (2 * depth + width)),
            transcendentals=count * units,
        ),
        name="expert_rest",
    )(rows, gate_early, up_early, gate_matrix, up_matrix, down_rest, down_other)


def pack_kernel(tokens, ids, weights, out):
    top, count = ids.shape
    experts = lax.broadcasted_iota(jnp.int32, (128, count), 0)
    hits = [(experts == ids[k : k + 1, :]).astype(jnp.float32) for k in range(top)]
    named = sum(hits).astype(jnp.bfloat16)
    row = lax.broadcasted_iota(jnp.int32, (count, count), 0)
    column = lax.broadcasted_iota(jnp.int32, (count, count), 1)
    before = matmul(named, (row < column).astype(jnp.bfloat16))
    ranks = [jnp.sum(hit * before, axis=0, keepdims=True) for hit in hits]
    routes = jnp.concatenate(
        [ids[...].astype(jnp.float32)]
        + ranks
        + [weights[...], jnp.zeros((128 - 3 * top, count), jnp.float32)],
        axis=0,
    ).astype(jnp.bfloat16)
    routes = lax.dot_general(
        (row == column).astype(jnp.bfloat16),
        routes,
        (((1,), (1,)), ((), ())),
        preferred_element_type=jnp.float32,
    ).astype(jnp.bfloat16)
    for group in range(out.shape[0]):
        start = group % 2 * HALF
        out[group, :, :HALF] = tokens[:, start : start + HALF]
        out[group, :, HALF:] = routes


def pack(tokens, expert_ids, combine, group_count):
    token_count, top_count = expert_ids.shape
    whole = pl.BlockSpec((top_count, token_count), lambda i: (0, 0))
    shape = (group_count, token_count, HALF + 128)
    return pl.pallas_call(
        pack_kernel,
        grid=(1,),
        in_specs=[pl.BlockSpec((token_count, BOTH), lambda i: (0, 0)), whole, whole],
        out_specs=pl.BlockSpec(shape, lambda i: (0, 0, 0)),
        out_shape=jax.ShapeDtypeStruct(shape, jnp.bfloat16),
        name="pack",
    )(tokens, expert_ids.T, combine.T)


def pick_kernel(top, rank_count, pair, routes, tokens, out, slots):
    tile = out.shape[0]
    step = pl.program_id(0)

    @pl.when(step == 0)
    def _():
        columns = routes.shape[1]
        row = lax.broadcasted_iota(jnp.int32, (columns, columns), 0)
        column = lax.broadcasted_iota(jnp.int32, (columns, columns), 1)
        turned = lax.dot_general(
            (row == column).astype(jnp.bfloat16),
            routes[...],
            (((1,), (1,)), ((), ())),
            preferred_element_type=jnp.float32,
        ).astype(jnp.int32)
        block, lanes, source_tokens = rank_count * 8, 32, 64
        source = lax.broadcasted_iota(jnp.int32, slots.shape, 1) // source_tokens
        expert = turned[:top] - pair[0] * lanes
        slots[...] = expert * block + source * rank_count + turned[top : 2 * top]

    rows = lax.broadcasted_iota(jnp.int32, (tile, slots.shape[1]), 0) + step * tile
    hit = rows == slots[0:1, :]
    for k in range(1, top):
        hit = hit | (rows == slots[k : k + 1, :])
    out[...] = matmul(hit.astype(jnp.bfloat16), tokens[...]).astype(jnp.bfloat16)


def pick(pair, first, tokens, width, slot_count, top_count):
    count = first.shape[0]
    tile = 256
    return pl.pallas_call(
        functools.partial(pick_kernel, top_count, CAP),
        grid=(slot_count // tile,),
        in_specs=[
            pl.BlockSpec(memory_space=pltpu.SMEM),
            pl.BlockSpec((count, 128), lambda i: (0, HALF // 128)),
            pl.BlockSpec((count, width), lambda i: (0, 0)),
        ],
        out_specs=pl.BlockSpec((tile, width), lambda i: (i, 0)),
        out_shape=pltpu.HBM((slot_count, width), jnp.bfloat16),
        scratch_shapes=[pltpu.VMEM((top_count, count), jnp.int32)],
        compiler_params=pltpu.CompilerParams(
            dimension_semantics=("arbitrary",), vmem_limit_bytes=24 * 1024 * 1024
        ),
        cost_estimate=pl.CostEstimate(
            flops=2 * slot_count * count * width,
            bytes_accessed=2 * width * (slot_count + count),
            transcendentals=0,
        ),
        name="pick",
    )(pair[None], first, tokens)


def shards(
    tokens, expert_ids, combine, hot_flags, gate_up_weight, gate_up_scale, down_weight, down_scale
):
    group_count = lax.axis_size("grp")
    lane_count = lax.axis_size("ex")
    token_count, model_width = tokens.shape
    top_count = expert_ids.shape[1]
    block = group_count * CAP
    slot_count = lane_count * block
    column_tokens = group_count * token_count
    own_grp = lax.axis_index("grp")
    own_pair = own_grp // 2
    parity = own_grp % 2
    partners = [(g, g ^ 1) for g in range(group_count)]

    first = pack(tokens, expert_ids, combine, group_count)
    first = lax.all_to_all(first, "grp", split_axis=0, concat_axis=0, tiled=True)
    first = first.reshape(column_tokens, HALF + 128)
    rest = lax.all_gather(tokens[:, BOTH:], "grp", axis=0, tiled=True)

    routes = first[:, HALF:]
    expert = routes[:, :top_count].astype(jnp.int32)
    rank = routes[:, top_count : 2 * top_count].astype(jnp.int32)
    weight = routes[:, 2 * top_count : 3 * top_count].astype(jnp.float32)
    source = jnp.arange(column_tokens, dtype=jnp.int32)[:, None] // token_count
    slot = (expert - own_pair * lane_count) * block + source * CAP + rank

    slots_across = lax.broadcasted_iota(jnp.int32, (column_tokens, slot_count), 1)
    mix = jnp.zeros((column_tokens, slot_count), jnp.float32)
    for k in range(top_count):
        mix = jnp.where(slot[:, k][:, None] == slots_across, weight[:, k][:, None], mix)
    mix = lax.optimization_barrier(mix.astype(jnp.bfloat16))

    is_hot = hot_flags[own_pair * lane_count + lax.axis_index("ex")] == 1
    group = model_width // gate_up_scale.shape[3]

    def dequantize_gate_up(j, start, stop):
        return dequantize(
            gate_up_weight[0, 0, j, start:stop],
            gate_up_scale[0, 0, j, start // group : stop // group],
            is_hot,
        )

    first_matrices = [dequantize_gate_up(j, 0, BOTH) for j in range(2)]
    rest_matrices = [dequantize_gate_up(j, BOTH, model_width) for j in range(2)]
    down_first = dequantize(
        down_weight[0, 0, :, :BOTH_BACK], down_scale[0, 0, :, :BOTH_BACK], is_hot
    )
    down_rest = dequantize(
        down_weight[0, 0, :, BOTH_BACK:], down_scale[0, 0, :, BOTH_BACK:], is_hot
    )

    def exchange(rows):
        return lax.all_to_all(
            rows.reshape(lane_count, block, -1), "ex", split_axis=0, concat_axis=0, tiled=True
        ).reshape(slot_count, -1)

    own_rows = pick(own_pair, first, first, HALF, slot_count, top_count)
    own_rows = exchange(own_rows)
    other_rows = lax.ppermute(own_rows, "grp", partners)
    rest_rows = pick(
        own_pair, first, rest, model_width - BOTH, slot_count, top_count
    )
    rest_rows = exchange(rest_rows)

    early = [
        matmul(own_rows, lax.dynamic_slice_in_dim(matrix, parity * HALF, HALF, 0))
        + matmul(other_rows, lax.dynamic_slice_in_dim(matrix, (1 - parity) * HALF, HALF, 0))
        for matrix in first_matrices
    ]
    early = lax.optimization_barrier(early)
    hidden, rest_rows, other_rows = expert_rest(
        rest_rows,
        *early,
        *rest_matrices,
        down_rest,
        lax.dynamic_slice_in_dim(down_first, (1 - parity) * HALF_BACK, HALF_BACK, 1),
    )
    rest_rows = exchange(rest_rows)
    partner_rows = lax.ppermute(other_rows, "grp", partners)
    own_rows = matmul(
        hidden, lax.dynamic_slice_in_dim(down_first, parity * HALF_BACK, HALF_BACK, 1)
    ).astype(jnp.bfloat16)
    own_rows = lax.optimization_barrier(own_rows)
    own_rows = own_rows.astype(jnp.float32) + partner_rows.astype(jnp.float32)
    own_rows = own_rows.astype(jnp.bfloat16)
    own_rows = exchange(own_rows)
    rest_sums = matmul(mix, rest_rows).astype(jnp.bfloat16)
    rest_out = lax.psum_scatter(rest_sums, "grp", scatter_dimension=0, tiled=True)
    own_sums = matmul(mix, own_rows).astype(jnp.bfloat16)
    own_sums = own_sums.reshape(group_count, token_count, HALF_BACK)
    sums = lax.all_to_all(own_sums, "grp", split_axis=0, concat_axis=0, tiled=True)
    sums = sums.reshape(group_count // 2, 2, token_count, HALF_BACK).astype(jnp.float32)
    sums = jnp.sum(sums, axis=0).astype(jnp.bfloat16)
    return jnp.concatenate([sums[0], sums[1], rest_out], axis=1)


def solution(mesh):
    return jax.shard_map(
        shards,
        mesh=mesh,
        in_specs=(
            P(("grp", "ex"), None),
            P(("grp", "ex"), None),
            P(("grp", "ex"), None),
            P(),
            P("grp", "ex", None, None, None),
            P("grp", "ex", None, None, None),
            P("grp", "ex", None, None),
            P("grp", "ex", None, None),
        ),
        out_specs=P(("grp", "ex"), None),
        check_vma=False,
    )
```
